32 devices in a mesh: row: 16 (over z, x, core), col: 2 (over y).
Axes of the slice: x: 2, y: 2, z: 4, core: 2. Of those that a mesh axis runs over, the one named last changes fastest.
Arguments:
- activations: bfloat16 [128, 16384], P('col', 'row'), may hold values from 0 to 2
- blocks_one: bfloat16 [16, 2, 64, 128, 128], P('row', 'col'), may hold values from -0.25 to 0.25
- pattern_one: int32 [16, 2, 64], P('row', 'col'), may hold values from 0 to 511, as said below
- count_one: int32 [16, 2], P('row', 'col'), may hold values from 1 to 64, as said below
- blocks_two: bfloat16 [2, 16, 64, 128, 128], P('col', 'row'), may hold values from -0.375 to 0.375
- pattern_two: int32 [2, 16, 64], P('col', 'row'), may hold values from 0 to 511, as said below
- count_two: int32 [2, 16], P('col', 'row'), may hold values from 1 to 64, as said below
Outputs:
- sparse_out: bfloat16 [128, 16384], P('col', 'row')
The draws below stay inside these ranges and needn't reach their ends.
Inputs may be any that keep to these rules, and one draw needn't show every extreme that they name: `pattern_one`: in each tile the slots below its count hold distinct positions; slots at or above the count hold positions in range whose blocks are not part of the weights. `count_one`: some tile has exactly 64 live slots. `pattern_two`: in each tile the slots below its count hold distinct positions; slots at or above the count hold positions in range whose blocks are not part of the weights. `count_two`: some tile has exactly 64 live slots.
All inputs are finite; a program needn't handle non-finite values.
Results may differ from the reference program's by a relative error of at most 0.0053.
Values may be sent and summed in bfloat16 or wider, within the bound.
No kernel may reach another device: no remote copies, remote signals or barrier semaphores. Data moves between devices by JAX's collectives and lax.ppermute only.
A program may use at most 64 MiB of HBM per device.

```python
import jax
import jax.numpy as jnp
from jax import lax

N = 16384
BLK = 128
MAXB = 64
ROWS = 128
BC_ONE = 64
BC_TWO = 8
TILE_SLOTS = 512
N_ROW = 16
N_COL = 2


def make_pattern(key, tiles):
    key_first = jax.random.fold_in(key, 11)
    key_second = jax.random.fold_in(key, 12)
    key_top = jax.random.fold_in(key, 13)
    key_place = jax.random.fold_in(key, 14)
    first = jax.random.randint(key_first, (tiles,), 0, MAXB)
    second = jax.random.randint(key_second, (tiles,), 0, MAXB)
    counts = 1 + first * second // MAXB
    top = jax.random.randint(key_top, (), 0, tiles)
    counts = jnp.where(jnp.arange(tiles) == top, MAXB, counts).astype(jnp.int32)
    keys = jax.random.split(key_place, tiles)
    places = jax.vmap(lambda k: jax.random.permutation(k, TILE_SLOTS)[:MAXB])(keys).astype(jnp.int32)
    return (places, counts)


def draw_pattern_one(key, part):
    places, counts = make_pattern(jax.random.fold_in(key, 1), N_ROW * N_COL)
    return places.reshape(N_ROW, N_COL, MAXB)


def draw_count_one(key, part):
    places, counts = make_pattern(jax.random.fold_in(key, 1), N_ROW * N_COL)
    return counts.reshape(N_ROW, N_COL)


def draw_pattern_two(key, part):
    places, counts = make_pattern(jax.random.fold_in(key, 2), N_COL * N_ROW)
    return places.reshape(N_COL, N_ROW, MAXB)


def draw_count_two(key, part):
    places, counts = make_pattern(jax.random.fold_in(key, 2), N_COL * N_ROW)
    return counts.reshape(N_COL, N_ROW)


def block_scale(rng, dims, cuts, smallest, largest):
    loudness = 1.0
    for dim, shards_of in cuts:
        steps = jax.random.uniform(jax.random.fold_in(jax.random.fold_in(rng, 6), dim), (shards_of,), jnp.float32, smallest / len(cuts), largest / len(cuts))
        loudness = loudness * jnp.repeat(jnp.exp(steps), dims[dim] // shards_of).reshape((-1,) + (1,) * (len(dims) - 1 - dim))
    return loudness


def normal_values(stream_key, extent, deviation, bound, cuts=(), held_as=jnp.bfloat16):
    entries = deviation * jax.random.normal(stream_key, extent, jnp.float32)
    if cuts:
        entries = entries * block_scale(stream_key, extent, cuts, -0.22, 0.18)
    return jnp.clip(entries, -bound, bound).astype(held_as)


def setup_inputs(seed: int = 0) -> dict:
    key_list = jax.random.split(jax.random.key(seed), 8)
    return {
        "activations": jnp.clip(2.0 * jax.random.uniform(key_list[0], (ROWS, N), jnp.float32) ** block_scale(key_list[0], (ROWS, N), ((0, 2), (1, 16)), -0.2, 0.2), 0.0, 2.0).astype(jnp.bfloat16),
        "blocks_one": normal_values(key_list[1], (N_ROW, N_COL, MAXB, BLK, BLK), (BLK * max(1, N_ROW * MAXB // (4 * BC_ONE))) ** -0.5, 0.25, ((0, 16), (1, 2))),
        "pattern_one": draw_pattern_one(jax.random.fold_in(key_list[7], 71), 0),
        "count_one": draw_count_one(jax.random.fold_in(key_list[7], 71), 0),
        "blocks_two": normal_values(key_list[4], (N_COL, N_ROW, MAXB, BLK, BLK), (BLK * max(1, N_COL * MAXB // (8 * BC_TWO))) ** -0.5, 0.375, ((0, 2), (1, 16))),
        "pattern_two": draw_pattern_two(jax.random.fold_in(key_list[7], 71), 0),
        "count_two": draw_count_two(jax.random.fold_in(key_list[7], 71), 0),
    }


bias_value = -0.3


def dense_tile(where, live, blocks, block_rows, block_cols):
    slots = blocks.shape[0]
    size = blocks.shape[-1]
    places = jnp.arange(block_rows * block_cols, dtype=jnp.int32)
    used = jnp.arange(slots, dtype=jnp.int32) < live
    onehot = ((where[:, None] == places[None, :]) & used[:, None]).astype(jnp.float32)
    tiles = jnp.einsum("st,sab->tab", onehot, blocks.astype(jnp.float32), precision=lax.Precision.HIGHEST)
    tiles = tiles.reshape(block_rows, block_cols, size, size).transpose(0, 2, 1, 3)
    return tiles.reshape(block_rows * size, block_cols * size)


def layer(act, where, live, blocks, parts_in, parts_out):
    size = blocks.shape[-1]
    in_width = N // parts_in
    out_width = N // parts_out
    block_rows = in_width // size
    block_cols = out_width // size

    def column(b):
        def add(acc, a):
            tile = dense_tile(where[a, b], live[a, b], blocks[a, b], block_rows, block_cols)
            left = lax.dynamic_slice_in_dim(act, a * in_width, in_width, 1).astype(jnp.float32)
            return acc + jnp.dot(left, tile, precision=lax.Precision.HIGHEST), None

        acc, _ = lax.scan(add, jnp.zeros((act.shape[0], out_width), jnp.float32), jnp.arange(parts_in, dtype=jnp.int32))
        return jnp.maximum(acc + bias_value, 0.0).astype(jnp.bfloat16)

    outs = lax.map(column, jnp.arange(parts_out, dtype=jnp.int32))
    return outs.transpose(1, 0, 2).reshape(act.shape[0], N)


def reference(activations, blocks_one, pattern_one, count_one, blocks_two, pattern_two, count_two):
    hidden = layer(activations, pattern_one, count_one, blocks_one, N_ROW, N_COL)
    return layer(hidden, pattern_two, count_two, blocks_two, N_COL, N_ROW)
```

```python
import functools

import jax
import jax.numpy as jnp
from jax import lax
from jax.experimental import pallas as pl
from jax.experimental.pallas import tpu as pltpu
from jax.sharding import PartitionSpec as P

bias_value = -0.3
CORES = 2
DEPTH = 4
UNROLL = 8
PARTS = 4
VMEM_BYTES = 40 * 1024 * 1024
SEND = jnp.float32


def digit_shift(sizes, which, by):
    total = sizes[0] * sizes[1] * sizes[2]
    stride = 1
    for size in sizes[which + 1 :]:
        stride *= size
    size = sizes[which]
    pairs = []
    for r in range(total):
        d = (r // stride) % size
        pairs.append((r, r + ((d + by) % size - d) * stride))
    return pairs


def first_kernel(sizes, groups, pattern, count, act, blocks, send, keep, stage, store, acc, sems):
    depth, width, cores = sizes
    slots, size, _ = blocks.shape
    rows = act.shape[0]
    units, m, _ = acc.shape
    units -= groups
    columns = units // groups
    per = slots // PARTS
    live = count[0, 0]
    copies = [
        pltpu.make_async_copy(blocks.at[pl.ds(i * per, per)], store.at[pl.ds(i * per, per)], sems.at[i])
        for i in range(PARTS)
    ]
    for copy in copies:
        copy.start()
    for r in range(act.shape[1] // size):
        stage[r] = act[:, r * size : (r + 1) * size]

    def clear(u, _):
        acc[u] = jnp.zeros((m, size), jnp.float32)
        return 0

    lax.fori_loop(0, units, clear, 0, unroll=8)
    for i in range(PARTS):
        copies[i].wait()

        def step(t, _):
            base = i * per + t * UNROLL
            found = []
            for j in range(UNROLL):
                place = pattern[0, base + j]
                product = jnp.dot(stage[place // columns], store[base + j], preferred_element_type=jnp.float32)
                found.append((place, product))
            for j, (place, product) in enumerate(found):
                used = base + j < live
                for g in range(groups):
                    at = jnp.where(used, g * columns + place % columns, units + g)
                    acc[at] += product[g * m : (g + 1) * m]
            return 0

        lax.fori_loop(0, jnp.clip((live - i * per + UNROLL - 1) // UNROLL, 0, per // UNROLL), step, 0)
    core = lax.axis_index("row") % cores
    half = units // cores
    mine = core * half
    other = (cores - 1 - core) * half

    def leave(u, _):
        send[u] = acc[other + u].astype(send.dtype)
        keep[u] = acc[mine + u]
        return 0

    lax.fori_loop(0, half, leave, 0, unroll=4)


def second_kernel(sizes, groups, pattern, count, *refs):
    depth, width, cores = sizes
    pieces = refs[: width * cores]
    blocks, out, hidden, acc, sems = refs[width * cores :]
    slots, size, _ = blocks.shape
    units, m, _ = hidden.shape
    columns = acc.shape[0] - 1
    rows_in = units // groups
    per = pieces[0].shape[0]
    each = per // depth
    copies = [
        pltpu.make_async_copy(piece, hidden.at[pl.ds(i * per, per)], sems.at[i]) for i, piece in enumerate(pieces)
    ]
    for copy in copies:
        copy.start()
    live = count[0, 0]
    row = lax.axis_index("row")
    core, x, z = row % cores, row // cores % width, row // (cores * width)
    for c in range(columns):
        acc[c] = jnp.zeros(acc.shape[1:], jnp.float32)

    def address(u):
        j = u % each
        zd = u // each % depth
        xd = u // per % width
        cd = u // (per * width)
        return (((core - cd + cores) % cores * width + (x - xd + width) % width) * depth + (z - zd + depth) % depth) * each + j

    for copy in copies:
        copy.wait()

    def step(t, _):
        base = t * UNROLL
        found = []
        for j in range(UNROLL):
            place = pattern[0, base + j]
            block = blocks[base + j]
            r = place // columns
            products = [
                jnp.dot(hidden[address(g * rows_in + r)], block, preferred_element_type=jnp.float32)
                for g in range(groups)
            ]
            found.append((place, products))
        for j, (place, products) in enumerate(found):
            at = jnp.where(base + j < live, place % columns, columns)
            for g, product in enumerate(products):
                acc[at, g * m : (g + 1) * m] += product
        return 0

    lax.fori_loop(0, (live + UNROLL - 1) // UNROLL, step, 0)
    for c in range(columns):
        out[:, c * size : (c + 1) * size] = acc[c].astype(out.dtype)


def shards(sizes, n_cols, activations, blocks_one, pattern_one, count_one, blocks_two, pattern_two, count_two):
    depth, width, cores = sizes
    n_rows = depth * width * cores
    own_rows, features = activations.shape
    slots, size = blocks_one.shape[2], blocks_one.shape[3]
    columns_one = features * n_rows // n_cols // size
    columns_two = features // size
    groups = max(1, n_rows // columns_one)
    units = columns_one * groups
    per = units // (width * cores)
    each = per // depth
    smem = pl.BlockSpec(memory_space=pltpu.SMEM)
    vmem = pl.BlockSpec(memory_space=pltpu.VMEM)
    anyspace = pl.BlockSpec(memory_space=pl.ANY)

    def move(value, which, by):
        return lax.ppermute(value, "row", digit_shift(sizes, which, by))

    def across(value, by):
        return lax.ppermute(value, "col", [(b, (b + by) % n_cols) for b in range(n_cols)])

    row = lax.axis_index("row")
    x, z = row // cores % width, row // (cores * width)

    def first(act):
        rows = act.shape[0]
        m = rows // groups
        half = (units // cores, m, size)
        return pl.pallas_call(
            functools.partial(first_kernel, sizes, groups),
            out_shape=(jax.ShapeDtypeStruct(half, SEND), jax.ShapeDtypeStruct(half, jnp.float32)),
            in_specs=[smem, smem, vmem, anyspace],
            out_specs=(vmem, vmem),
            scratch_shapes=[
                pltpu.VMEM((columns_two, rows, size), jnp.bfloat16),
                pltpu.VMEM((slots, size, size), jnp.bfloat16),
                pltpu.VMEM((units + groups, m, size), jnp.float32),
                pltpu.SemaphoreType.DMA((PARTS,)),
            ],
            compiler_params=pltpu.CompilerParams(vmem_limit_bytes=VMEM_BYTES),
            name="first",
        )(pattern_one.reshape(1, slots), count_one, act, blocks_one.reshape(slots, size, size))

    def pick(arrays, at):
        total = lax.dynamic_index_in_dim(arrays[0], at, 0, keepdims=False)
        for a in arrays[1:]:
            total = total + lax.dynamic_index_in_dim(a, at, 0, keepdims=False).astype(jnp.float32)
        return total

    def reduce_core(pair):
        send, keep = pair
        shape = (width, per) + keep.shape[1:]
        return [keep.reshape(shape), move(send, 2, 1).reshape(shape)]

    def reduce_width(arrays):
        gets = [move(pick(arrays, (x + k) % width).astype(jnp.bfloat16), 1, k) for k in range(1, width)]
        arrays = [pick(arrays, x)] + gets
        return [a.reshape((depth, each) + a.shape[1:]) for a in arrays]

    def reduce_depth(arrays):
        gets = [move(pick(arrays, (z + k) % depth).astype(jnp.bfloat16), 0, k) for k in range(1, depth)]
        total = pick(arrays, z)
        for g in gets:
            total = total + g.astype(jnp.float32)
        return jnp.maximum(total + bias_value, 0.0).astype(jnp.bfloat16)

    def gather_depth(hidden):
        return jnp.concatenate([hidden] + [move(hidden, 0, k) for k in range(1, depth)], axis=0)

    def gather_width(line):
        pieces = [line] + [move(line, 1, k) for k in range(1, width)]
        return pieces + [move(p, 2, k) for k in range(1, cores) for p in pieces]

    def second(pieces, out_type):
        m = pieces[0].shape[1]
        rows = m * groups
        return pl.pallas_call(
            functools.partial(second_kernel, sizes, groups),
            out_shape=jax.ShapeDtypeStruct((rows, features), out_type),
            in_specs=[smem, smem] + [anyspace] * len(pieces) + [vmem],
            out_specs=vmem,
            scratch_shapes=[
                pltpu.VMEM((units, m, size), jnp.bfloat16),
                pltpu.VMEM((columns_two + 1, rows, size), jnp.float32),
                pltpu.SemaphoreType.DMA((len(pieces),)),
            ],
            compiler_params=pltpu.CompilerParams(vmem_limit_bytes=VMEM_BYTES),
            name="second",
        )(pattern_two.reshape(1, slots), count_two, *pieces, blocks_two.reshape(slots, size, size))

    theirs = [across(activations, k) for k in range(1, n_cols)]
    theirs = theirs[0] if n_cols == 2 else jnp.concatenate(theirs, axis=0)
    chunks = [activations, theirs]
    for stage in (first, reduce_core, reduce_width, reduce_depth, gather_depth, gather_width):
        chunks = [stage(c) for c in chunks]
    mine = second(chunks[0], jnp.float32)
    rest = second(chunks[1], jnp.bfloat16)
    for k in range(1, n_cols):
        back = across(lax.slice_in_dim(rest, (k - 1) * own_rows, k * own_rows, axis=0), -k)
        mine = mine + back.astype(jnp.float32)
    return jnp.maximum(mine + bias_value, 0.0).astype(jnp.bfloat16)


def solution(mesh):
    n_rows, n_cols = mesh.shape["row"], mesh.shape["col"]
    sizes = (DEPTH, n_rows // (DEPTH * CORES), CORES)
    in_specs = (
        P("col", "row"),
        P("row", "col", None, None, None),
        P("row", "col", None),
        P("row", "col"),
        P("col", "row", None, None, None),
        P("col", "row", None),
        P("col", "row"),
    )
    return jax.shard_map(
        functools.partial(shards, sizes, n_cols),
        mesh=mesh,
        in_specs=in_specs,
        out_specs=P("col", "row"),
        check_vma=False,
    )
```

```python
import functools

import jax
import jax.numpy as jnp
from jax import lax
from jax.experimental import pallas as pl
from jax.experimental.pallas import tpu as pltpu
from jax.sharding import PartitionSpec as P


bias_value = -0.3
CORES = 2
DEPTH = 4
UNROLL = 8
SEND = jnp.float32
SPARE = 1024 * 1024


def split(value, by):
    if by & (by - 1) == 0:
        return lax.shift_right_logical(value, by.bit_length() - 1), value & (by - 1)
    return value // by, value % by


def turned(digit, by, size):
    if size & (size - 1) == 0:
        return digit ^ by
    return (digit + by) % size


def behind(here, there, size):
    if size & (size - 1) == 0:
        return here ^ there
    return (here - there + size) % size


def digit_shift(sizes, which, by):
    total = sizes[0] * sizes[1] * sizes[2]
    stride = 1
    for size in sizes[which + 1 :]:
        stride *= size
    size = sizes[which]
    pairs = []
    for r in range(total):
        d = (r // stride) % size
        pairs.append((r, r + (turned(d, by, size) - d) * stride))
    return pairs


def first_kernel(sizes, groups, load, pattern, count, act, blocks, *refs):
    _, _, cores = sizes
    _, size, _ = blocks.shape
    if load:
        send, keep, held, stage, acc, sems = refs
        copies = [
            pltpu.make_async_copy(act.at[:, pl.ds(r * size, size)], stage.at[r], sems.at[r])
            for r in range(stage.shape[0])
        ]
        copies.append(pltpu.make_async_copy(blocks, held, sems.at[stage.shape[0]]))
        for copy in copies:
            copy.start()
        blocks = held
    else:
        send, keep, stage, acc = refs
    units, m, _ = acc.shape
    units -= groups
    columns = units // groups
    live = count[0, 0]
    if not load:
        for r in range(stage.shape[0]):
            stage[r] = act[:, r * size : (r + 1) * size]

    def clear(u, _):
        acc[u] = jnp.zeros((m, size), jnp.float32)
        return 0

    lax.fori_loop(0, units, clear, 0, unroll=8)
    if load:
        for copy in copies:
            copy.wait()

    def step(t, _):
        base = t * UNROLL
        found = []
        for j in range(UNROLL):
            r, c = split(pattern[0, base + j], columns)
            product = jnp.dot(stage[r], blocks[base + j], preferred_element_type=jnp.float32)
            found.append((c, product))
        for j, (c, product) in enumerate(found):
            used = base + j < live
            for g in range(groups):
                at = jnp.where(used, g * columns + c, units + g)
                acc[at] += product[g * m : (g + 1) * m]
        return 0

    lax.fori_loop(0, (live + UNROLL - 1) // UNROLL, step, 0)
    core = lax.axis_index("row") % cores
    half = units // cores
    mine = core * half
    other = (cores - 1 - core) * half

    def leave(u, _):
        send[u] = acc[other + u].astype(send.dtype)
        keep[u] = acc[mine + u]
        return 0

    lax.fori_loop(0, half, leave, 0, unroll=4)


def spread_kernel(sizes, which, *refs):
    size = sizes[which]
    arrays, outs = refs[:-size], refs[-size:]
    stride = 1
    for s in sizes[which + 1 :]:
        stride *= s
    here = lax.axis_index("row") // stride % size

    def step(j, _):
        for k, out in enumerate(outs):
            at = turned(here, k, size)
            total = arrays[0][at, j]
            for a in arrays[1:]:
                total = total + a[at, j].astype(jnp.float32)
            out[j] = total.astype(out.dtype)
        return 0

    lax.fori_loop(0, outs[0].shape[0], step, 0, unroll=2)


def finish_kernel(*refs):
    def step(j, _):
        total = refs[0][j]
        for a in refs[1:-1]:
            total = total + a[j].astype(jnp.float32)
        refs[-1][j] = jnp.maximum(total + bias_value, 0.0).astype(jnp.bfloat16)
        return 0

    lax.fori_loop(0, refs[0].shape[0], step, 0, unroll=True if refs[0].shape[0] < 8 else 4)


def join_kernel(*refs):
    n = refs[0].shape[0]
    for i, ref in enumerate(refs[:-1]):
        for j in range(n):
            refs[-1][i * n + j] = ref[j]


def second_kernel(sizes, groups, pattern, count, *refs):
    depth, width, cores = sizes
    pieces = refs[: width * cores]
    blocks, out, acc = refs[width * cores :]
    _, size, _ = blocks.shape
    per, m, _ = pieces[0].shape
    columns = acc.shape[0] - 1
    rows_in = per * width * cores // groups
    each = per // depth
    live = count[0, 0]
    row = lax.axis_index("row")
    core, x, z = row % cores, row // cores % width, row // (cores * width)
    for c in range(columns):
        acc[c] = jnp.zeros(acc.shape[1:], jnp.float32)

    def hidden(u):
        rest, j = split(u, each)
        rest, zd = split(rest, depth)
        cd, xd = split(rest, width)
        piece = behind(core, cd, cores) * width + behind(x, xd, width)
        at = behind(z, zd, depth) * each + j
        found = pieces[0][at]
        for i in range(1, len(pieces)):
            found = jnp.where(piece == i, pieces[i][at], found)
        return found

    def step(t, _):
        base = t * UNROLL
        found = []
        for j in range(UNROLL):
            block = blocks[base + j]
            r, c = split(pattern[0, base + j], columns)
            products = [
                jnp.dot(hidden(g * rows_in + r), block, preferred_element_type=jnp.float32) for g in range(groups)
            ]
            found.append((c, products))
        for j, (c, products) in enumerate(found):
            at = jnp.where(base + j < live, c, columns)
            for g, product in enumerate(products):
                acc[at, g * m : (g + 1) * m] += product
        return 0

    lax.fori_loop(0, (live + UNROLL - 1) // UNROLL, step, 0)
    for c in range(columns):
        out[:, c * size : (c + 1) * size] = acc[c].astype(out.dtype)


def shards(sizes, n_cols, activations, blocks_one, pattern_one, count_one, blocks_two, pattern_two, count_two):
    depth, width, cores = sizes
    n_rows = depth * width * cores
    own_rows, features = activations.shape
    slots, size = blocks_one.shape[2], blocks_one.shape[3]
    columns_one = features * n_rows // n_cols // size
    columns_two = features // size
    groups = max(1, n_rows // columns_one)
    units = columns_one * groups
    per = units // (width * cores)
    each = per // depth
    smem = pl.BlockSpec(memory_space=pltpu.SMEM)
    vmem = pl.BlockSpec(memory_space=pltpu.VMEM)
    anyspace = pl.BlockSpec(memory_space=pl.ANY)

    def move(value, which, by):
        return lax.ppermute(value, "row", digit_shift(sizes, which, by))

    def across(value, by):
        return lax.ppermute(value, "col", [(b, (b + by) % n_cols) for b in range(n_cols)])

    def call(kernel, outs, scalars, arrays, scratch=(), rows=0, load=0):
        total = sum(a.size * a.dtype.itemsize for a in (*arrays, *outs, *scratch))
        cost = None
        if rows:
            cost = pl.CostEstimate(
                flops=2 * slots * rows * size * size, bytes_accessed=slots * size * size * 2, transcendentals=0
            )
        return pl.pallas_call(
            kernel,
            out_shape=tuple(outs),
            in_specs=[smem] * len(scalars) + [anyspace if load else vmem] * len(arrays),
            out_specs=(vmem,) * len(outs),
            scratch_shapes=[pltpu.VMEM(a.shape, a.dtype) for a in scratch] + [pltpu.SemaphoreType.DMA((load,))] * bool(load),
            compiler_params=pltpu.CompilerParams(vmem_limit_bytes=total + SPARE),
            cost_estimate=cost,
        )(*scalars, *arrays)

    def first(act, stored):
        load = stored is None
        rows = act.shape[0]
        m = rows // groups
        half = (units // cores, m, size)
        outs = [jax.ShapeDtypeStruct(half, SEND), jax.ShapeDtypeStruct(half, jnp.float32)]
        if load:
            act = pltpu.with_memory_space_constraint(act, pltpu.HBM)
            stored = pltpu.with_memory_space_constraint(blocks_one.reshape(slots, size, size), pltpu.HBM)
            outs.append(jax.ShapeDtypeStruct(stored.shape, stored.dtype))
        return call(
            functools.partial(first_kernel, sizes, groups, load),
            outs,
            [pattern_one.reshape(1, slots), count_one],
            [act, stored],
            [
                jax.ShapeDtypeStruct((columns_two, rows, size), jnp.bfloat16),
                jax.ShapeDtypeStruct((units + groups, m, size), jnp.float32),
            ],
            rows,
            (columns_two + 1) * load,
        )

    def spread(arrays, which):
        n = sizes[which]
        arrays = [a.reshape((n, a.shape[0] // n) + a.shape[1:]) for a in arrays]
        shape = arrays[0].shape[1:]
        kinds = [jnp.float32] + [jnp.bfloat16] * (n - 1)
        outs = call(
            functools.partial(spread_kernel, sizes, which),
            [jax.ShapeDtypeStruct(shape, kind) for kind in kinds],
            [],
            arrays,
        )
        return [outs[0]] + [move(out, which, k + 1) for k, out in enumerate(outs[1:])]

    def reduce_core(pair):
        send, keep = pair
        return [keep, move(send, 2, 1)]

    def reduce_width(arrays):
        return spread(arrays, 1)

    def reduce_depth(arrays):
        arrays = spread(arrays, 0)
        return call(finish_kernel, [jax.ShapeDtypeStruct(arrays[0].shape, jnp.bfloat16)], [], arrays)[0]

    def gather_depth(hidden):
        arrays = [hidden] + [move(hidden, 0, k) for k in range(1, depth)]
        joined = (depth * each,) + hidden.shape[1:]
        return call(join_kernel, [jax.ShapeDtypeStruct(joined, jnp.bfloat16)], [], arrays)[0]

    def gather_width(line):
        far = [move(line, 1, k) for k in range(1, width)]
        near = [move(line, 2, k) for k in range(1, cores)]
        return [line, *far] + [p for k in range(1, cores) for p in (near[k - 1], *(move(f, 2, k) for f in far))]

    def second(pieces, out_type):
        rows = pieces[0].shape[1] * groups
        return call(
            functools.partial(second_kernel, sizes, groups),
            [jax.ShapeDtypeStruct((rows, features), out_type)],
            [pattern_two.reshape(1, slots), count_two],
            [*pieces, blocks_two.reshape(slots, size, size)],
            [jax.ShapeDtypeStruct((columns_two + 1, rows, size), jnp.float32)],
            rows if out_type == jnp.bfloat16 else 0,
        )[0]

    theirs = [across(activations, k) for k in range(1, n_cols)]
    theirs = theirs[0] if n_cols == 2 else jnp.concatenate(theirs, axis=0)
    send, keep, stored = first(activations, None)
    own = (send, keep)
    theirs = first(theirs, stored)
    chunks = {"theirs": theirs, "own": own}
    stages = {
        "reduce_core": reduce_core,
        "reduce_width": reduce_width,
        "reduce_depth": reduce_depth,
        "gather_depth": gather_depth,
        "gather_width": gather_width,
    }
    for run in stages.values():
        for name in chunks:
            chunks[name] = run(chunks[name])
    rest = second(chunks["theirs"], jnp.bfloat16)
    mine = second(chunks["own"], jnp.float32)
    for k in range(1, n_cols):
        back = across(lax.slice_in_dim(rest, (k - 1) * own_rows, k * own_rows, axis=0), -k)
        mine = mine + back.astype(jnp.float32)
    return jnp.maximum(mine + bias_value, 0.0).astype(jnp.bfloat16)


def solution(mesh):
    n_rows, n_cols = mesh.shape["row"], mesh.shape["col"]
    sizes = (DEPTH, n_rows // (DEPTH * CORES), CORES)
    in_specs = (
        P("col", "row"),
        P("row", "col", None, None, None),
        P("row", "col", None),
        P("row", "col"),
        P("col", "row", None, None, None),
        P("col", "row", None),
        P("col", "row"),
    )
    return jax.shard_map(
        functools.partial(shards, sizes, n_cols),
        mesh=mesh,
        in_specs=in_specs,
        out_specs=P("col", "row"),
        check_vma=False,
    )
```

```python
import functools

import jax
import jax.numpy as jnp
from jax import lax
from jax.experimental import pallas as pl
from jax.experimental.pallas import tpu as pltpu
from jax.sharding import PartitionSpec as P


bias_value = -0.3
CORES = 2
DEPTH = 4
UNROLL = 16
SEND = jnp.float32
SPARE = 1024 * 1024


def split(value, by):
    if by & (by - 1) == 0:
        return lax.shift_right_logical(value, by.bit_length() - 1), value & (by - 1)
    return value // by, value % by


def turned(digit, by, size):
    if size & (size - 1) == 0:
        return digit ^ by
    return (digit + by) % size


def sender(digit, by, size):
    if size & (size - 1) == 0:
        return digit ^ by
    return (digit + size - by) % size


def digit_shift(sizes, which, by):
    total = sizes[0] * sizes[1] * sizes[2]
    stride = 1
    for size in sizes[which + 1 :]:
        stride *= size
    size = sizes[which]
    pairs = []
    for r in range(total):
        d = (r // stride) % size
        pairs.append((r, r + (turned(d, by, size) - d) * stride))
    return pairs


def first_kernel(sizes, groups, load, pattern, count, act, blocks, *refs):
    _, width, cores = sizes
    _, size, _ = blocks.shape
    if load:
        held, stage, acc, sems = refs[2 * width :]
        copies = [
            pltpu.make_async_copy(act.at[:, pl.ds(r * size, size)], stage.at[r], sems.at[r])
            for r in range(stage.shape[0])
        ]
        copies.append(pltpu.make_async_copy(blocks, held, sems.at[stage.shape[0]]))
        for copy in copies:
            copy.start()
        blocks = held
    else:
        stage, acc = refs[2 * width :]
    units, m, _ = acc.shape
    units -= groups
    columns = units // groups
    live = count[0, 0]
    if not load:
        for r in range(stage.shape[0]):
            stage[r] = act[:, r * size : (r + 1) * size]

    def clear(u, _):
        acc[u] = jnp.zeros((m, size), jnp.float32)
        return 0

    lax.fori_loop(0, units, clear, 0, unroll=8)
    if load:
        for copy in copies:
            copy.wait()

    def step(t, _):
        base = t * UNROLL
        found = []
        for j in range(UNROLL):
            r, c = split(pattern[0, base + j], columns)
            product = jnp.dot(stage[r], blocks[base + j], preferred_element_type=jnp.float32)
            found.append((c, product))
        for j, (c, product) in enumerate(found):
            used = base + j < live
            for g in range(groups):
                at = jnp.where(used, g * columns + c, units + g)
                acc[at] += product[g * m : (g + 1) * m]
        return 0

    lax.fori_loop(0, (live + UNROLL - 1) // UNROLL, step, 0)
    row = lax.axis_index("row")
    core, x = row % cores, row // cores % width
    per = units // (cores * width)
    for k in range(width):
        xd = turned(x, k, width)
        mine = (core * width + xd) * per
        other = ((cores - 1 - core) * width + xd) * per
        send, keep = refs[k], refs[width + k]

        def leave(u, _):
            send[u] = acc[other + u].astype(send.dtype)
            keep[u] = acc[mine + u]
            return 0

        lax.fori_loop(0, per, leave, 0, unroll=4)


def pair_kernel(left, right, out):
    def step(j, _):
        out[j] = (left[j] + right[j].astype(jnp.float32)).astype(out.dtype)
        return 0

    lax.fori_loop(0, out.shape[0], step, 0, unroll=4)


def spread_kernel(size, stride, *refs):
    arrays, outs = refs[:-size], refs[-size:]
    here = lax.axis_index("row") // stride % size

    def step(j, _):
        for k, out in enumerate(outs):
            at = turned(here, k, size)
            total = arrays[0][at, j]
            for a in arrays[1:]:
                total = total + a[at, j].astype(jnp.float32)
            out[j] = total.astype(out.dtype)
        return 0

    lax.fori_loop(0, outs[0].shape[0], step, 0, unroll=2)


def finish_kernel(*refs):
    def step(j, _):
        total = refs[0][j]
        for a in refs[1:-1]:
            total = total + a[j].astype(jnp.float32)
        refs[-1][j] = jnp.maximum(total + bias_value, 0.0).astype(jnp.bfloat16)
        return 0

    lax.fori_loop(0, refs[0].shape[0], step, 0, unroll=True if refs[0].shape[0] < 8 else 4)


def join_kernel(*refs):
    n = refs[0].shape[0]
    for i, ref in enumerate(refs[:-1]):
        for j in range(n):
            refs[-1][i * n + j] = ref[j]


def second_kernel(sizes, groups, pattern, count, *refs):
    depth, width, cores = sizes
    pieces = refs[: width * cores]
    blocks, out, hidden, acc = refs[width * cores :]
    _, size, _ = blocks.shape
    units, m, _ = hidden.shape
    columns = acc.shape[0] - 1
    rows_in = units // groups
    each = units // (depth * width * cores)
    live = count[0, 0]
    row = lax.axis_index("row")
    core, x, z = row % cores, row // cores % width, row // (cores * width)
    for c in range(columns):
        acc[c] = jnp.zeros(acc.shape[1:], jnp.float32)
    for i, piece in enumerate(pieces):
        cd, xd = sender(core, i // width, cores), sender(x, i % width, width)
        for k in range(depth):
            base = ((cd * width + xd) * depth + sender(z, k, depth)) * each
            for j in range(each):
                hidden[base + j] = piece[k * each + j]

    def step(t, _):
        base = t * UNROLL
        found = []
        for j in range(UNROLL):
            block = blocks[base + j]
            r, c = split(pattern[0, base + j], columns)
            products = [
                jnp.dot(hidden[g * rows_in + r], block, preferred_element_type=jnp.float32) for g in range(groups)
            ]
            found.append((c, products))
        for j, (c, products) in enumerate(found):
            at = jnp.where(base + j < live, c, columns)
            for g, product in enumerate(products):
                acc[at, g * m : (g + 1) * m] += product
        return 0

    lax.fori_loop(0, (live + UNROLL - 1) // UNROLL, step, 0)
    for c in range(columns):
        out[:, c * size : (c + 1) * size] = acc[c].astype(out.dtype)


def shards(sizes, n_cols, activations, blocks_one, pattern_one, count_one, blocks_two, pattern_two, count_two):
    depth, width, cores = sizes
    n_rows = depth * width * cores
    own_rows, features = activations.shape
    slots, size = blocks_one.shape[2], blocks_one.shape[3]
    columns_one = features * n_rows // n_cols // size
    columns_two = features // size
    groups = max(1, n_rows // columns_one)
    units = columns_one * groups
    per = units // (width * cores)
    each = per // depth
    smem = pl.BlockSpec(memory_space=pltpu.SMEM)
    vmem = pl.BlockSpec(memory_space=pltpu.VMEM)
    anyspace = pl.BlockSpec(memory_space=pl.ANY)

    def move(value, which, by):
        return lax.ppermute(value, "row", digit_shift(sizes, which, by))

    def across(value, by):
        return lax.ppermute(value, "col", [(b, (b + by) % n_cols) for b in range(n_cols)])

    def call(kernel, outs, scalars, arrays, scratch=(), rows=0, load=0):
        total = sum(a.size * a.dtype.itemsize for a in (*arrays, *outs, *scratch))
        cost = None
        if rows:
            cost = pl.CostEstimate(
                flops=2 * slots * rows * size * size, bytes_accessed=slots * size * size * 2, transcendentals=0
            )
        return pl.pallas_call(
            kernel,
            out_shape=tuple(outs),
            in_specs=[smem] * len(scalars) + [anyspace if load else vmem] * len(arrays),
            out_specs=(vmem,) * len(outs),
            scratch_shapes=[pltpu.VMEM(a.shape, a.dtype) for a in scratch] + [pltpu.SemaphoreType.DMA((load,))] * bool(load),
            compiler_params=pltpu.CompilerParams(vmem_limit_bytes=total + SPARE),
            cost_estimate=cost,
        )(*scalars, *arrays)

    def first(act, stored):
        load = stored is None
        rows = act.shape[0]
        m = rows // groups
        shape = (per, m, size)
        outs = [jax.ShapeDtypeStruct(shape, kind) for kind in (SEND, jnp.float32) for _ in range(width)]
        if load:
            act = pltpu.with_memory_space_constraint(act, pltpu.HBM)
            stored = pltpu.with_memory_space_constraint(blocks_one.reshape(slots, size, size), pltpu.HBM)
            outs.append(jax.ShapeDtypeStruct(stored.shape, stored.dtype))
        return call(
            functools.partial(first_kernel, sizes, groups, load),
            outs,
            [pattern_one.reshape(1, slots), count_one],
            [act, stored],
            [
                jax.ShapeDtypeStruct((columns_two, rows, size), jnp.bfloat16),
                jax.ShapeDtypeStruct((units + groups, m, size), jnp.float32),
            ],
            rows,
            (columns_two + 1) * load,
        )

    def reduce_core(arrays):
        steps = [*range(1, width), 0]
        got = {}
        for k in steps:
            got[k] = move(arrays[k], 2, 1)
        return [(arrays[width + k], got[k]) for k in range(width)]

    def reduce_width(pairs):
        gets = []
        for k in range(1, width):
            out = jax.ShapeDtypeStruct(pairs[k][0].shape, jnp.bfloat16)
            gets.append(move(call(pair_kernel, [out], [], pairs[k])[0], 1, k))
        return [*pairs[0], *gets]

    def reduce_depth(arrays):
        arrays = [a.reshape((depth, each) + a.shape[1:]) for a in arrays]
        kinds = [jnp.float32] + [jnp.bfloat16] * (depth - 1)
        outs = [jax.ShapeDtypeStruct(arrays[0].shape[1:], kind) for kind in kinds]
        outs = call(functools.partial(spread_kernel, depth, width * cores), outs, [], arrays)
        arrays = [outs[0]] + [move(out, 0, k + 1) for k, out in enumerate(outs[1:])]
        return call(finish_kernel, [jax.ShapeDtypeStruct(arrays[0].shape, jnp.bfloat16)], [], arrays)[0]

    def gather_depth(hidden):
        arrays = [hidden] + [move(hidden, 0, k) for k in range(1, depth)]
        joined = (depth * each,) + hidden.shape[1:]
        return call(join_kernel, [jax.ShapeDtypeStruct(joined, jnp.bfloat16)], [], arrays)[0]

    def gather_width(line):
        far = [move(line, 1, k) for k in range(1, width)]
        near = [move(line, 2, k) for k in range(1, cores)]
        return [line, *far] + [p for k in range(1, cores) for p in (near[k - 1], *(move(f, 2, k) for f in far))]

    def second(pieces, out_type):
        rows = pieces[0].shape[1] * groups
        return call(
            functools.partial(second_kernel, sizes, groups),
            [jax.ShapeDtypeStruct((rows, features), out_type)],
            [pattern_two.reshape(1, slots), count_two],
            [*pieces, blocks_two.reshape(slots, size, size)],
            [
                jax.ShapeDtypeStruct((units, rows // groups, size), jnp.bfloat16),
                jax.ShapeDtypeStruct((columns_two + 1, rows, size), jnp.float32),
            ],
            rows if out_type == jnp.bfloat16 else 0,
        )[0]

    theirs = [across(activations, k) for k in range(1, n_cols)]
    theirs = theirs[0] if n_cols == 2 else jnp.concatenate(theirs, axis=0)
    *own, stored = first(activations, None)
    theirs = first(theirs, stored)
    chunks = {"theirs": theirs, "own": own}
    stages = {
        "reduce_core": reduce_core,
        "reduce_width": reduce_width,
        "reduce_depth": reduce_depth,
        "gather_depth": gather_depth,
        "gather_width": gather_width,
    }
    for run in stages.values():
        for name in chunks:
            chunks[name] = run(chunks[name])
    rest = second(chunks["theirs"], jnp.bfloat16)
    mine = second(chunks["own"], jnp.float32)
    for k in range(1, n_cols):
        back = across(lax.slice_in_dim(rest, (k - 1) * own_rows, k * own_rows, axis=0), -k)
        mine = mine + back.astype(jnp.float32)
    return jnp.maximum(mine + bias_value, 0.0).astype(jnp.bfloat16)


def solution(mesh):
    n_rows, n_cols = mesh.shape["row"], mesh.shape["col"]
    sizes = (DEPTH, n_rows // (DEPTH * CORES), CORES)
    in_specs = (
        P("col", "row"),
        P("row", "col", None, None, None),
        P("row", "col", None),
        P("row", "col"),
        P("col", "row", None, None, None),
        P("col", "row", None),
        P("col", "row"),
    )
    return jax.shard_map(
        functools.partial(shards, sizes, n_cols),
        mesh=mesh,
        in_specs=in_specs,
        out_specs=P("col", "row"),
        check_vma=False,
    )
```

```python
import functools
import math

import jax
import jax.numpy as jnp
from jax import lax
from jax.experimental import pallas as pl
from jax.experimental.pallas import tpu as pltpu
from jax.sharding import PartitionSpec as P


bias_value = -0.3
CORES = 2
DEPTH = 4
STEP_BYTES = 2 * 1024 * 1024
SEND = jnp.float32
SPARE = 1024 * 1024
PLANS = 2
CUTS = 2


def slots_a_step(slots, rows, size):
    step = slots
    while step > 8 and step * rows * size * 4 > STEP_BYTES:
        step //= 2
    return step


def split(value, by):
    if by & (by - 1) == 0:
        return lax.shift_right_logical(value, by.bit_length() - 1), value & (by - 1)
    return value // by, value % by


def turned(digit, by, size):
    if size & (size - 1) == 0:
        return digit ^ by
    return (digit + by) % size


def sender(digit, by, size):
    if size & (size - 1) == 0:
        return digit ^ by
    return (digit + size - by) % size


def digit_shift(sizes, which, by):
    total = sizes[0] * sizes[1] * sizes[2]
    stride = 1
    for size in sizes[which + 1 :]:
        stride *= size
    size = sizes[which]
    pairs = []
    for r in range(total):
        d = (r // stride) % size
        pairs.append((r, r + (turned(d, by, size) - d) * stride))
    return pairs


def first_kernel(sizes, groups, load, *refs):
    _, width, cores = sizes
    if load:
        count, plans, (act, blocks), refs = refs[0], refs[1 : 1 + PLANS], refs[1 + PLANS : 3 + PLANS], refs[3 + PLANS :]
        held, *here, stage, acc, sems = refs[2 * width :]
        slots, size, _ = blocks.shape
        moves = [(plan, there) for plan, there in zip(plans, here)]
        moves += [(act.at[:, pl.ds(r * size, size)], stage.at[r]) for r in range(stage.shape[0])]
        moves.append((blocks, held))
        copies = [pltpu.make_async_copy(a, b, sems.at[i]) for i, (a, b) in enumerate(moves)]
        for copy in copies:
            copy.start()
        for copy in copies[:PLANS]:
            copy.wait()
        copies = copies[PLANS:]
        blocks = held
        pattern = here[0]
    else:
        pattern, count, act, blocks = refs[:4]
        refs = refs[4:]
        slots, size, _ = blocks.shape
        stage, acc = refs[2 * width :]
    units, m, _ = acc.shape
    units -= groups
    columns = units // groups
    unroll = slots_a_step(slots, m * groups, size)
    live = count[0, 0]
    if not load:
        for r in range(stage.shape[0]):
            stage[r] = act[:, r * size : (r + 1) * size]

    def clear(u, _):
        acc[u] = jnp.zeros((m, size), jnp.float32)
        return 0

    lax.fori_loop(0, units, clear, 0, unroll=8)
    if load:
        for copy in copies:
            copy.wait()

    def step(t, _):
        base = t * unroll
        found = []
        for j in range(unroll):
            r, c = split(pattern[0, base + j], columns)
            product = jnp.dot(stage[r], blocks[base + j], preferred_element_type=jnp.float32)
            found.append((c, product))
        for j, (c, product) in enumerate(found):
            used = base + j < live
            for g in range(groups):
                at = jnp.where(used, g * columns + c, units + g)
                acc[at] += product[g * m : (g + 1) * m]
        return 0

    lax.fori_loop(0, (live + unroll - 1) // unroll, step, 0)
    row = lax.axis_index("row")
    core, x = row % cores, row // cores % width
    per = units // (cores * width)
    for k in range(width):
        xd = turned(x, k, width)
        mine = (core * width + xd) * per
        other = ((cores - 1 - core) * width + xd) * per
        send, keep = refs[k], refs[width + k]

        def leave(u, _):
            send[u] = acc[other + u].astype(send.dtype)
            keep[u] = acc[mine + u]
            return 0

        lax.fori_loop(0, per, leave, 0, unroll=4)


def pair_kernel(left, right, out):
    def step(j, _):
        out[j] = (left[j] + right[j].astype(jnp.float32)).astype(out.dtype)
        return 0

    lax.fori_loop(0, out.shape[0], step, 0, unroll=4)


def spread_kernel(size, stride, *refs):
    arrays, outs = refs[:-size], refs[-size:]
    here = lax.axis_index("row") // stride % size

    def step(j, _):
        for k, out in enumerate(outs):
            at = turned(here, k, size)
            total = arrays[0][at, j]
            for a in arrays[1:]:
                total = total + a[at, j].astype(jnp.float32)
            out[j] = total.astype(out.dtype)
        return 0

    lax.fori_loop(0, outs[0].shape[0], step, 0, unroll=2)


def finish_kernel(*refs):
    def step(j, _):
        total = refs[0][j]
        for a in refs[1:-1]:
            total = total + a[j].astype(jnp.float32)
        refs[-1][j] = jnp.maximum(total + bias_value, 0.0).astype(jnp.bfloat16)
        return 0

    lax.fori_loop(0, refs[0].shape[0], step, 0, unroll=True if refs[0].shape[0] < 8 else 4)


def join_kernel(cuts, *refs):
    arrays, outs = refs[:-cuts], refs[-cuts:]
    n = arrays[0].shape[0]
    m = outs[0].shape[1]
    for h, out in enumerate(outs):
        for i, ref in enumerate(arrays):
            for j in range(n):
                out[i * n + j] = ref[j, h * m : (h + 1) * m]


def second_kernel(sizes, groups, pattern, count, *refs):
    depth, width, cores = sizes
    pieces = refs[: width * cores]
    blocks, out, hidden, acc = refs[width * cores :]
    slots, size, _ = blocks.shape
    units, m, _ = hidden.shape
    columns = acc.shape[0] - 1
    rows_in = units // groups
    unroll = slots_a_step(slots, m * groups, size)
    each = units // (depth * width * cores)
    live = count[0, 0]
    row = lax.axis_index("row")
    core, x, z = row % cores, row // cores % width, row // (cores * width)
    for c in range(columns):
        acc[c] = jnp.zeros(acc.shape[1:], jnp.float32)
    for i, piece in enumerate(pieces):
        cd, xd = sender(core, i // width, cores), sender(x, i % width, width)
        for k in range(depth):
            base = ((cd * width + xd) * depth + sender(z, k, depth)) * each
            for j in range(each):
                hidden[base + j] = piece[k * each + j]

    def step(t, _):
        base = t * unroll
        found = []
        for j in range(unroll):
            block = blocks[base + j]
            r, c = split(pattern[0, base + j], columns)
            products = [
                jnp.dot(hidden[g * rows_in + r], block, preferred_element_type=jnp.float32) for g in range(groups)
            ]
            found.append((c, products))
        for j, (c, products) in enumerate(found):
            at = jnp.where(base + j < live, c, columns)
            for g, product in enumerate(products):
                acc[at, g * m : (g + 1) * m] += product
        return 0

    lax.fori_loop(0, (live + unroll - 1) // unroll, step, 0)
    for c in range(columns):
        out[:, c * size : (c + 1) * size] = acc[c].astype(out.dtype)


def shards(sizes, n_cols, activations, blocks_one, pattern_one, count_one, blocks_two, pattern_two, count_two):
    depth, width, cores = sizes
    n_rows = depth * width * cores
    own_rows, features = activations.shape
    slots, size = blocks_one.shape[2], blocks_one.shape[3]
    columns_one = features * n_rows // n_cols // size
    columns_two = features // size
    groups = max(1, n_rows // columns_one)
    cuts = CUTS if n_cols == 2 and groups == 1 else 1
    units = columns_one * groups
    per = units // (width * cores)
    each = per // depth
    smem = pl.BlockSpec(memory_space=pltpu.SMEM)
    vmem = pl.BlockSpec(memory_space=pltpu.VMEM)
    anyspace = pl.BlockSpec(memory_space=pl.ANY)

    def move(value, which, by):
        return lax.ppermute(value, "row", digit_shift(sizes, which, by))

    def across(value, by):
        return lax.ppermute(value, "col", [(b, (b + by) % n_cols) for b in range(n_cols)])

    def call(kernel, outs, scalars, arrays, scratch=(), rows=0, copies=0, tables=0):
        total = sum(math.prod(a.shape) * a.dtype.itemsize for a in (*arrays, *outs, *scratch))
        cost = None
        if rows:
            cost = pl.CostEstimate(
                flops=2 * slots * rows * size * size, bytes_accessed=slots * size * size * 2, transcendentals=0
            )
        return pl.pallas_call(
            kernel,
            out_shape=tuple(outs),
            in_specs=[smem] * len(scalars) + [anyspace if copies else vmem] * len(arrays),
            out_specs=(vmem,) * (len(outs) - tables) + (smem,) * tables,
            scratch_shapes=[pltpu.VMEM(a.shape, a.dtype) for a in scratch]
            + [pltpu.SemaphoreType.DMA((copies,))] * bool(copies),
            compiler_params=pltpu.CompilerParams(vmem_limit_bytes=total + SPARE),
            cost_estimate=cost,
        )(*scalars, *arrays)

    def first(act, plans, stored=None):
        load = stored is None
        rows = act.shape[0]
        m = rows // groups
        shape = (per, m, size)
        outs = [jax.ShapeDtypeStruct(shape, kind) for kind in (SEND, jnp.float32) for _ in range(width)]
        scratch = [
            jax.ShapeDtypeStruct((columns_two, rows, size), jnp.bfloat16),
            jax.ShapeDtypeStruct((units + groups, m, size), jnp.float32),
        ]
        kernel = functools.partial(first_kernel, sizes, groups, load)
        if not load:
            return call(kernel, outs, [plans[0], count_one], [act, stored], scratch, rows)
        arrays = [*plans, act, blocks_one.reshape(slots, size, size)]
        arrays = [pltpu.with_memory_space_constraint(a, pltpu.HBM) for a in arrays]
        outs.append(jax.ShapeDtypeStruct(arrays[-1].shape, jnp.bfloat16))
        outs += [pltpu.SMEM(p.shape, p.dtype) for p in plans]
        return call(kernel, outs, [count_one], arrays, scratch, rows, columns_two + 1 + PLANS, PLANS)

    def reduce_core(arrays):
        steps = [*range(1, width), 0]
        got = {}
        for k in steps:
            got[k] = move(arrays[k], 2, 1)
        return [(arrays[width + k], got[k]) for k in range(width)]

    def reduce_width(pairs):
        gets = []
        for k in range(1, width):
            out = jax.ShapeDtypeStruct(pairs[k][0].shape, jnp.bfloat16)
            gets.append(move(call(pair_kernel, [out], [], pairs[k])[0], 1, k))
        return [*pairs[0], *gets]

    def reduce_depth(arrays):
        arrays = [a.reshape((depth, each) + a.shape[1:]) for a in arrays]
        kinds = [jnp.float32] + [jnp.bfloat16] * (depth - 1)
        outs = [jax.ShapeDtypeStruct(arrays[0].shape[1:], kind) for kind in kinds]
        outs = call(functools.partial(spread_kernel, depth, width * cores), outs, [], arrays)
        arrays = [outs[0]] + [move(out, 0, k + 1) for k, out in enumerate(outs[1:])]
        return call(finish_kernel, [jax.ShapeDtypeStruct(arrays[0].shape, jnp.bfloat16)], [], arrays)[0]

    def gather_depth(hidden, cuts):
        arrays = [hidden] + [move(hidden, 0, k) for k in range(1, depth)]
        joined = (depth * each, hidden.shape[1] // cuts, hidden.shape[2])
        outs = [jax.ShapeDtypeStruct(joined, jnp.bfloat16)] * cuts
        return call(functools.partial(join_kernel, cuts), outs, [], arrays)

    def gather_width(line):
        far = [move(line, 1, k) for k in range(1, width)]
        near = [move(line, 2, k) for k in range(1, cores)]
        return [line, *far] + [p for k in range(1, cores) for p in (near[k - 1], *(move(f, 2, k) for f in far))]

    def second(pieces, plans, out_type):
        rows = pieces[0].shape[1] * groups
        return call(
            functools.partial(second_kernel, sizes, groups),
            [jax.ShapeDtypeStruct((rows, features), out_type)],
            [plans[1], count_two],
            [*pieces, blocks_two.reshape(slots, size, size)],
            [
                jax.ShapeDtypeStruct((units, rows // groups, size), jnp.bfloat16),
                jax.ShapeDtypeStruct((columns_two + 1, rows, size), jnp.float32),
            ],
            rows if out_type == jnp.bfloat16 else 0,
        )[0]

    theirs = [across(activations, k) for k in range(1, n_cols)]
    theirs = theirs[0] if n_cols == 2 else jnp.concatenate(theirs, axis=0)
    plans = [pattern_one.reshape(1, slots), pattern_two.reshape(1, slots)]
    *own, stored, plan_one, plan_two = first(activations, plans)
    plans = [plan_one, plan_two]
    theirs = first(theirs, plans, stored)
    chunks = {"theirs": theirs, "own": own}
    stages = {
        "reduce_core": reduce_core,
        "reduce_width": reduce_width,
        "reduce_depth": reduce_depth,
    }
    for run in stages.values():
        for name in chunks:
            chunks[name] = run(chunks[name])
    lines = gather_depth(chunks["theirs"], cuts)
    own_line = gather_depth(chunks["own"], 1)[0]
    rest = []
    for line in lines:
        pieces = gather_width(line)
        rest.append(second(pieces, plans, jnp.bfloat16))
    pieces = gather_width(own_line)
    mine = second(pieces, plans, jnp.float32)
    for k in range(1, n_cols):
        back = []
        for part in rest:
            rows = own_rows if cuts == 1 else part.shape[0]
            back.append(across(lax.slice_in_dim(part, (k - 1) * rows, k * rows, axis=0), -k))
        back = back[0] if cuts == 1 else jnp.concatenate(back, axis=0)
        mine = mine + back.astype(jnp.float32)
    return jnp.maximum(mine + bias_value, 0.0).astype(jnp.bfloat16)


def solution(mesh):
    n_rows, n_cols = mesh.shape["row"], mesh.shape["col"]
    sizes = (DEPTH, n_rows // (DEPTH * CORES), CORES)
    in_specs = (
        P("col", "row"),
        P("row", "col", None, None, None),
        P("row", "col", None),
        P("row", "col"),
        P("col", "row", None, None, None),
        P("col", "row", None),
        P("col", "row"),
    )
    return jax.shard_map(
        functools.partial(shards, sizes, n_cols),
        mesh=mesh,
        in_specs=in_specs,
        out_specs=P("col", "row"),
        check_vma=False,
    )
```

```python
import functools
import math

import jax
import jax.numpy as jnp
from jax import lax
from jax.experimental import pallas as pl
from jax.experimental.pallas import tpu as pltpu
from jax.sharding import PartitionSpec as P


bias_value = -0.3
CORES = 2
DEPTH = 4
STEP_BYTES = 2 * 1024 * 1024
SEND = jnp.float32
SPARE = 1024 * 1024
PLANS = 2


def slots_a_step(slots, rows, size):
    step = slots
    while step > 8 and step * rows * size * 4 > STEP_BYTES:
        step //= 2
    return step


def split(value, by):
    if by & (by - 1) == 0:
        return lax.shift_right_logical(value, by.bit_length() - 1), value & (by - 1)
    return value // by, value % by


def turned(digit, by, size):
    if size & (size - 1) == 0:
        return digit ^ by
    return (digit + by) % size


def sender(digit, by, size):
    if size & (size - 1) == 0:
        return digit ^ by
    return (digit + size - by) % size


def digit_shift(sizes, which, by):
    total = sizes[0] * sizes[1] * sizes[2]
    stride = 1
    for size in sizes[which + 1 :]:
        stride *= size
    size = sizes[which]
    pairs = []
    for r in range(total):
        d = (r // stride) % size
        pairs.append((r, r + (turned(d, by, size) - d) * stride))
    return pairs


def first_kernel(sizes, groups, load, *refs):
    _, width, cores = sizes
    if load:
        count, plans, (act, blocks), refs = refs[0], refs[1 : 1 + PLANS], refs[1 + PLANS : 3 + PLANS], refs[3 + PLANS :]
        held, *here, stage, acc, sems = refs[2 * width :]
        slots, size, _ = blocks.shape
        moves = [(plan, there) for plan, there in zip(plans, here)]
        moves += [(act.at[:, pl.ds(r * size, size)], stage.at[r]) for r in range(stage.shape[0])]
        moves.append((blocks, held))
        copies = [pltpu.make_async_copy(a, b, sems.at[i]) for i, (a, b) in enumerate(moves)]
        for copy in copies:
            copy.start()
        for copy in copies[:PLANS]:
            copy.wait()
        copies = copies[PLANS:]
        blocks = held
        pattern = here[0]
    else:
        pattern, count, act, blocks = refs[:4]
        refs = refs[4:]
        slots, size, _ = blocks.shape
        stage, acc = refs[2 * width :]
    units, m, _ = acc.shape
    units -= groups
    columns = units // groups
    unroll = slots_a_step(slots, m * groups, size)
    live = count[0, 0]
    if not load:
        for r in range(stage.shape[0]):
            stage[r] = act[:, r * size : (r + 1) * size]

    def clear(u, _):
        acc[u] = jnp.zeros((m, size), jnp.float32)
        return 0

    lax.fori_loop(0, units, clear, 0, unroll=8)
    if load:
        for copy in copies:
            copy.wait()

    def step(t, _):
        base = t * unroll
        found = []
        for j in range(unroll):
            r, c = split(pattern[0, base + j], columns)
            product = jnp.dot(stage[r], blocks[base + j], preferred_element_type=jnp.float32)
            found.append((c, product))
        for j, (c, product) in enumerate(found):
            used = base + j < live
            for g in range(groups):
                at = jnp.where(used, g * columns + c, units + g)
                acc[at] += product[g * m : (g + 1) * m]
        return 0

    lax.fori_loop(0, (live + unroll - 1) // unroll, step, 0)
    row = lax.axis_index("row")
    core, x = row % cores, row // cores % width
    per = units // (cores * width)
    for k in range(width):
        xd = turned(x, k, width)
        mine = (core * width + xd) * per
        other = ((cores - 1 - core) * width + xd) * per
        send, keep = refs[k], refs[width + k]

        def leave(u, _):
            send[u] = acc[other + u].astype(send.dtype)
            keep[u] = acc[mine + u]
            return 0

        lax.fori_loop(0, per, leave, 0, unroll=4)


def pair_kernel(left, right, out):
    def step(j, _):
        out[j] = (left[j] + right[j].astype(jnp.float32)).astype(out.dtype)
        return 0

    lax.fori_loop(0, out.shape[0], step, 0, unroll=4)


def spread_kernel(size, stride, *refs):
    arrays, outs = refs[:-size], refs[-size:]
    here = lax.axis_index("row") // stride % size

    def step(j, _):
        for k, out in enumerate(outs):
            at = turned(here, k, size)
            total = arrays[0][at, j]
            for a in arrays[1:]:
                total = total + a[at, j].astype(jnp.float32)
            out[j] = total.astype(out.dtype)
        return 0

    lax.fori_loop(0, outs[0].shape[0], step, 0, unroll=2)


def finish_kernel(*refs):
    def step(j, _):
        total = refs[0][j]
        for a in refs[1:-1]:
            total = total + a[j].astype(jnp.float32)
        refs[-1][j] = jnp.maximum(total + bias_value, 0.0).astype(jnp.bfloat16)
        return 0

    lax.fori_loop(0, refs[0].shape[0], step, 0, unroll=True if refs[0].shape[0] < 8 else 4)


def join_kernel(*refs):
    n = refs[0].shape[0]
    for i, ref in enumerate(refs[:-1]):
        for j in range(n):
            refs[-1][i * n + j] = ref[j]


def second_kernel(sizes, groups, pattern, count, *refs):
    depth, width, cores = sizes
    pieces = refs[: width * cores]
    blocks, out, hidden, acc = refs[width * cores :]
    slots, size, _ = blocks.shape
    units, m, _ = hidden.shape
    columns = acc.shape[0] - 1
    rows_in = units // groups
    unroll = slots_a_step(slots, m * groups, size)
    each = units // (depth * width * cores)
    live = count[0, 0]
    row = lax.axis_index("row")
    core, x, z = row % cores, row // cores % width, row // (cores * width)
    for c in range(columns):
        acc[c] = jnp.zeros(acc.shape[1:], jnp.float32)
    for i, piece in enumerate(pieces):
        cd, xd = sender(core, i // width, cores), sender(x, i % width, width)
        for k in range(depth):
            base = ((cd * width + xd) * depth + sender(z, k, depth)) * each
            for j in range(each):
                hidden[base + j] = piece[k * each + j]

    def step(t, _):
        base = t * unroll
        found = []
        for j in range(unroll):
            block = blocks[base + j]
            r, c = split(pattern[0, base + j], columns)
            products = [
                jnp.dot(hidden[g * rows_in + r], block, preferred_element_type=jnp.float32) for g in range(groups)
            ]
            found.append((c, products))
        for j, (c, products) in enumerate(found):
            at = jnp.where(base + j < live, c, columns)
            for g, product in enumerate(products):
                acc[at, g * m : (g + 1) * m] += product
        return 0

    lax.fori_loop(0, (live + unroll - 1) // unroll, step, 0)
    for c in range(columns):
        out[:, c * size : (c + 1) * size] = acc[c].astype(out.dtype)


def shards(sizes, n_cols, activations, blocks_one, pattern_one, count_one, blocks_two, pattern_two, count_two):
    depth, width, cores = sizes
    n_rows = depth * width * cores
    own_rows, features = activations.shape
    slots, size = blocks_one.shape[2], blocks_one.shape[3]
    columns_one = features * n_rows // n_cols // size
    columns_two = features // size
    groups = max(1, n_rows // columns_one)
    units = columns_one * groups
    per = units // (width * cores)
    each = per // depth
    smem = pl.BlockSpec(memory_space=pltpu.SMEM)
    vmem = pl.BlockSpec(memory_space=pltpu.VMEM)
    anyspace = pl.BlockSpec(memory_space=pl.ANY)

    def move(value, which, by):
        return lax.ppermute(value, "row", digit_shift(sizes, which, by))

    def across(value, by):
        return lax.ppermute(value, "col", [(b, (b + by) % n_cols) for b in range(n_cols)])

    def call(kernel, outs, scalars, arrays, scratch=(), rows=0, copies=0, tables=0):
        total = sum(math.prod(a.shape) * a.dtype.itemsize for a in (*arrays, *outs, *scratch))
        cost = None
        if rows:
            cost = pl.CostEstimate(
                flops=2 * slots * rows * size * size, bytes_accessed=slots * size * size * 2, transcendentals=0
            )
        return pl.pallas_call(
            kernel,
            out_shape=tuple(outs),
            in_specs=[smem] * len(scalars) + [anyspace if copies else vmem] * len(arrays),
            out_specs=(vmem,) * (len(outs) - tables) + (smem,) * tables,
            scratch_shapes=[pltpu.VMEM(a.shape, a.dtype) for a in scratch]
            + [pltpu.SemaphoreType.DMA((copies,))] * bool(copies),
            compiler_params=pltpu.CompilerParams(vmem_limit_bytes=total + SPARE),
            cost_estimate=cost,
        )(*scalars, *arrays)

    def first(act, plans, stored=None):
        load = stored is None
        rows = act.shape[0]
        m = rows // groups
        shape = (per, m, size)
        outs = [jax.ShapeDtypeStruct(shape, kind) for kind in (SEND, jnp.float32) for _ in range(width)]
        scratch = [
            jax.ShapeDtypeStruct((columns_two, rows, size), jnp.bfloat16),
            jax.ShapeDtypeStruct((units + groups, m, size), jnp.float32),
        ]
        kernel = functools.partial(first_kernel, sizes, groups, load)
        if not load:
            return call(kernel, outs, [plans[0], count_one], [act, stored], scratch, rows)
        arrays = [*plans, act, blocks_one.reshape(slots, size, size)]
        arrays = [pltpu.with_memory_space_constraint(a, pltpu.HBM) for a in arrays]
        outs.append(jax.ShapeDtypeStruct(arrays[-1].shape, jnp.bfloat16))
        outs += [pltpu.SMEM(p.shape, p.dtype) for p in plans]
        return call(kernel, outs, [count_one], arrays, scratch, rows, columns_two + 1 + PLANS, PLANS)

    def reduce_core(arrays):
        steps = [*range(1, width), 0]
        got = {}
        for k in steps:
            got[k] = move(arrays[k], 2, 1)
        return [(arrays[width + k], got[k]) for k in range(width)]

    def reduce_width(pairs):
        gets = []
        for k in range(1, width):
            out = jax.ShapeDtypeStruct(pairs[k][0].shape, jnp.bfloat16)
            gets.append(move(call(pair_kernel, [out], [], pairs[k])[0], 1, k))
        return [*pairs[0], *gets]

    def reduce_depth(arrays):
        arrays = [a.reshape((depth, each) + a.shape[1:]) for a in arrays]
        kinds = [jnp.float32] + [jnp.bfloat16] * (depth - 1)
        outs = [jax.ShapeDtypeStruct(arrays[0].shape[1:], kind) for kind in kinds]
        outs = call(functools.partial(spread_kernel, depth, width * cores), outs, [], arrays)
        arrays = [outs[0]] + [move(out, 0, k + 1) for k, out in enumerate(outs[1:])]
        return call(finish_kernel, [jax.ShapeDtypeStruct(arrays[0].shape, jnp.bfloat16)], [], arrays)[0]

    def gather_depth(hidden):
        arrays = [hidden] + [move(hidden, 0, k) for k in range(1, depth)]
        joined = (depth * each,) + hidden.shape[1:]
        return call(join_kernel, [jax.ShapeDtypeStruct(joined, jnp.bfloat16)], [], arrays)[0]

    def gather_width(line):
        far = [move(line, 1, k) for k in range(1, width)]
        near = [move(line, 2, k) for k in range(1, cores)]
        return [line, *far] + [p for k in range(1, cores) for p in (near[k - 1], *(move(f, 2, k) for f in far))]

    def second(pieces, plans, out_type):
        rows = pieces[0].shape[1] * groups
        return call(
            functools.partial(second_kernel, sizes, groups),
            [jax.ShapeDtypeStruct((rows, features), out_type)],
            [plans[1], count_two],
            [*pieces, blocks_two.reshape(slots, size, size)],
            [
                jax.ShapeDtypeStruct((units, rows // groups, size), jnp.bfloat16),
                jax.ShapeDtypeStruct((columns_two + 1, rows, size), jnp.float32),
            ],
            rows if out_type == jnp.bfloat16 else 0,
        )[0]

    theirs = [across(activations, k) for k in range(1, n_cols)]
    theirs = theirs[0] if n_cols == 2 else jnp.concatenate(theirs, axis=0)
    plans = [pattern_one.reshape(1, slots), pattern_two.reshape(1, slots)]
    *own, stored, plan_one, plan_two = first(activations, plans)
    plans = [plan_one, plan_two]
    theirs = first(theirs, plans, stored)
    chunks = {"theirs": theirs, "own": own}
    stages = {
        "reduce_core": reduce_core,
        "reduce_width": reduce_width,
        "reduce_depth": reduce_depth,
        "gather_depth": gather_depth,
        "gather_width": gather_width,
    }
    for run in stages.values():
        for name in chunks:
            chunks[name] = run(chunks[name])
    rest = second(chunks["theirs"], plans, jnp.bfloat16)
    mine = second(chunks["own"], plans, jnp.float32)
    for k in range(1, n_cols):
        back = across(lax.slice_in_dim(rest, (k - 1) * own_rows, k * own_rows, axis=0), -k)
        mine = mine + back.astype(jnp.float32)
    return jnp.maximum(mine + bias_value, 0.0).astype(jnp.bfloat16)


def solution(mesh):
    n_rows, n_cols = mesh.shape["row"], mesh.shape["col"]
    sizes = (DEPTH, n_rows // (DEPTH * CORES), CORES)
    in_specs = (
        P("col", "row"),
        P("row", "col", None, None, None),
        P("row", "col", None),
        P("row", "col"),
        P("col", "row", None, None, None),
        P("col", "row", None),
        P("col", "row"),
    )
    return jax.shard_map(
        functools.partial(shards, sizes, n_cols),
        mesh=mesh,
        in_specs=in_specs,
        out_specs=P("col", "row"),
        check_vma=False,
    )
```
